32 devices in a mesh: replica: 8 (over z, core), fsdp: 4 (over y, x).
Axes of the slice: x: 2, y: 2, z: 4, core: 2. Of those that a mesh axis runs over, the one named last changes fastest.
Arguments:
- acts: bfloat16 [1, 4096, 8192], P(None, ('replica', 'fsdp')), may hold values from -6 to 6
- key_cot: bfloat16 [1, 4096, 512], P(None, ('replica', 'fsdp')), may hold values from -0.29882812 to 0.29882812
- params: float32 [8192, 512], P('fsdp'), may hold values from -4 to 4
- moment_one: float32 [8192, 512], P('fsdp'), may hold values from -1.8 to 1.8
- moment_two: float32 [8192, 512], P('fsdp'), may hold values from 0.05 to 2
- outer_mom: float32 [8192, 512], P(('fsdp', 'replica')), may hold values from -1.8 to 1.8
Outputs:
- new_params: float32 [8192, 512], P(('fsdp', 'replica'))
- new_mom: float32 [8192, 512], P(('fsdp', 'replica'))
The draws below stay inside these ranges and needn't reach their ends.
All inputs are finite; a program needn't handle non-finite values.
Results may differ from the reference program's by a relative error of at most 0.0007.
Values may be sent and summed in bfloat16 or wider, within the bound.
A program may use at most 64 MiB of HBM per device.

```python
import math
import jax
import jax.numpy as jnp
from jax import lax

D = 8192
KVW = 512
TOK_DEV = 128
MICRO = 1
TOKENS = 4096
N_REPLICA = 8
N_FSDP = 4


def strengthened(values, rng, source, target, blocks, factor):
    owner, partner = [(jnp.arange(values.shape[dim]) // (values.shape[dim] // blocks)).reshape([-1 if axis == dim else 1 for axis in range(values.ndim)]) for dim in (source, target)]
    chosen = jax.random.permutation(rng, blocks)[partner]
    strong = (owner == chosen) | (owner == (partner + blocks // 2) % blocks)
    return jnp.where(strong, factor * values, values)


def block_levels(rng, extent, shards, low, high):
    level = 1.0
    for axis_at, blocks in shards:
        heights = jax.random.uniform(jax.random.fold_in(jax.random.fold_in(rng, 6), axis_at), (blocks,), jnp.float32, low / len(shards), high / len(shards))
        level = level * jnp.repeat(jnp.exp(heights), extent[axis_at] // blocks).reshape((-1,) + (1,) * (len(extent) - 1 - axis_at))
    return level


def bell_draw(own_key, shape, spread, most, cuts=(), held_as=jnp.bfloat16):
    level = block_levels(own_key, shape, cuts, -0.22, 0.18) if cuts else 1.0
    values = jax.random.normal(own_key, shape, jnp.float32) * spread * level
    return jnp.minimum(jnp.maximum(values, -most), most).astype(held_as)


def bell_draw_with(stream_key, shape, spread, bound, shards, heavy, held_as=jnp.bfloat16):
    drawn = spread * jax.random.normal(stream_key, shape, jnp.float32)
    if shards:
        drawn = drawn * block_levels(stream_key, shape, shards, -0.22, 0.18)
    return jnp.clip(strengthened(drawn, jax.random.fold_in(stream_key, 3), *heavy), -bound, bound).astype(held_as)


def setup_inputs(seed: int = 0) -> dict:
    splits = jax.random.split(jax.random.key(seed), 7)
    return {
        "acts": bell_draw_with(splits[0], (MICRO, TOKENS, D), 1.0, 6.0, ((1, 32),), (1, 2, 32, 2.75)),
        "key_cot": bell_draw(splits[1], (MICRO, TOKENS, KVW), 0.05, 0.29882812, ((1, 32),)),
        "params": bell_draw(splits[2], (D, KVW), 1.0, 4.0, ((0, 4),), jnp.float32),
        "moment_one": bell_draw(splits[3], (D, KVW), 0.3, 1.8, ((0, 4),), jnp.float32),
        "moment_two": jnp.clip(jnp.exp(math.log(2.0) - 3.6888794 * jax.random.uniform(splits[4], (D, KVW), jnp.float32) ** block_levels(splits[4], (D, KVW), ((0, 4),), -0.2, 0.2)), 0.05, 2.0),
        "outer_mom": bell_draw(splits[5], (D, KVW), 0.3, 1.8, ((0, 32),), jnp.float32),
    }


beta_one = 0.9
beta_two = 0.95
epsilon = 1e-08
inner_rate = 0.3
decay_rate = 0.1
outer_rate = 0.7
momentum = 0.9

def adamw_step(weights, first, second, gradient):
    first = beta_one * first + (1.0 - beta_one) * gradient
    second = beta_two * second + (1.0 - beta_two) * gradient * gradient
    weights = weights - inner_rate * (first / (jnp.sqrt(second) + epsilon) + decay_rate * weights)
    return (weights, first, second)

def reference(acts, key_cot, params, moment_one, moment_two, outer_mom):
    group_rows = TOK_DEV * N_FSDP

    def one_worker(running, worker):
        start_row = (worker * group_rows).astype(jnp.int32)
        inputs = lax.dynamic_slice_in_dim(acts, start_row, group_rows, 1).astype(jnp.float32)
        cotangent = lax.dynamic_slice_in_dim(key_cot, start_row, group_rows, 1).astype(jnp.float32)
        gradients = jnp.einsum('mtd,mtk->mdk', inputs, cotangent)
        weights, first, second = (params, moment_one, moment_two)
        for number in range(MICRO):
            weights, first, second = adamw_step(weights, first, second, gradients[number])
        return (running + (params - weights), None)
    summed, _ = lax.scan(one_worker, jnp.zeros(params.shape, jnp.float32), jnp.arange(N_REPLICA, dtype=jnp.int32))
    drift_mean = summed / N_REPLICA
    new_mom = momentum * outer_mom + drift_mean
    new_params = params - outer_rate * (drift_mean + momentum * new_mom)
    return (new_params, new_mom)
```

```python
import functools

import jax
import jax.numpy as jnp
from jax import lax
from jax.experimental import pallas as pl
from jax.experimental.pallas import tpu as pltpu
from jax.sharding import PartitionSpec as P

beta_one = 0.9
beta_two = 0.95
epsilon = 1e-08
inner_rate = 0.3
decay_rate = 0.1
outer_rate = 0.7
momentum = 0.9

MESH = pl.DeviceIdType.MESH
OUTER_PLAN = (
    (3, 0, 1, 3, None), (2, 0, 2, 2, None), (3, 1, 1, 3, None), (2, 1, 1, 2, None),
    (1, 0, 1, 0, None), (1, 1, 1, 0, None), (0, 0, None, None, None), (0, 1, None, None, None),
)
INNER_PLAN = (
    (3, 0, 3, 1, None), (1, 0, 1, 0, None), (2, 0, 2, 1, (3, 0)), (1, 1, 1, 0, None),
    (2, 1, 2, 1, (3, 1)), (3, 1, 3, 1, (2, 1)), (0, 0, None, None, None), (0, 1, None, None, None),
)
UNIT = 128
WINDOW = 5
EARLY = 1
AFTER = 4

def adamw_direction(first, second, gradient):
    first = beta_one * first + (1.0 - beta_one) * gradient
    second = beta_two * second + (1.0 - beta_two) * gradient * gradient
    return first / (jnp.sqrt(second) + epsilon)

def kernel(
    n_rep,
    acts_ref, cot_ref, params_ref, first_ref, second_ref, outer_ref, new_params_ref, new_mom_ref,
    acts_buf, cot_buf, first_buf, second_buf, pair_out, pair_in, far_out, far_in, stash, anchor_buf, outer_buf,
    acts_recv, cot_recv, pair_recv, far_recv, send_sem, local_sem,
):
    rep = lax.axis_index("replica")
    shard = lax.axis_index("fsdp")
    line, core = lax.div(rep, 2), lax.rem(rep, 2)
    row_at, col_at = lax.div(shard, 2), lax.rem(shard, 2)
    rows = first_ref.shape[0]
    block = rows // n_rep
    size = block // 2
    half = cot_ref.shape[0] // 2
    tokens = acts_buf.shape[0] * acts_buf.shape[1]
    width = cot_buf.shape[2]
    partner = line * 2 + (1 - core)
    shards = (shard, row_at * 2 + (1 - col_at), (1 - row_at) * 2 + col_at, (1 - row_at) * 2 + (1 - col_at))
    lines = (line, line + 1 - 2 * lax.rem(line, 2), lax.rem(line + 2, 4), 3 - line)
    outer = 1 - lax.rem(lax.div(line, 2) + lax.rem(line, 2), 2)
    is_outer = outer == 1
    is_inner = jnp.logical_not(is_outer)

    def span(start, length):
        return pl.ds(pl.multiple_of(start, length), length)

    def remote(source, target, send, recv, device):
        return pltpu.make_async_remote_copy(
            src_ref=source, dst_ref=target, send_sem=send, recv_sem=recv, device_id=device, device_id_type=MESH
        )

    def pick(at_outer, at_inner):
        return outer * at_outer + (1 - outer) * at_inner

    units = []
    for step, (at_outer, at_inner) in enumerate(zip(OUTER_PLAN, INNER_PLAN)):
        other = pick(lines[at_outer[0]], lines[at_inner[0]])
        start = pick(at_outer[1], at_inner[1]) * size
        for h, owner in ((0, 1 - core), (1, core)):
            units.append((step, h, (other * 2 + owner) * block + start))

    barrier = pltpu.get_barrier_semaphore()
    peers = [(rep, shards[d]) for d in (3, 1, 2)] + [(partner, shard)]
    peers += [(lines[o] * 2 + core, shard) for o in (1, 2)]
    for peer in peers:
        pl.semaphore_signal(barrier, inc=1, device_id=peer, device_id_type=MESH)

    @pl.when(is_inner)
    def _():
        pl.semaphore_signal(barrier, inc=1, device_id=(lines[3] * 2 + core, shard), device_id_type=MESH)

    local = [
        pltpu.make_async_copy(cot_ref, cot_buf.at[0], local_sem.at[0]),
        pltpu.make_async_copy(acts_ref.at[:, span(shard * rows, rows)], acts_buf.at[0], local_sem.at[1]),
        pltpu.make_async_copy(first_ref, first_buf, local_sem.at[2]),
        pltpu.make_async_copy(second_ref, second_buf, local_sem.at[3]),
    ]
    finals = [
        pltpu.make_async_copy(params_ref.at[span(rep * block, block)], anchor_buf, local_sem.at[4]),
        pltpu.make_async_copy(outer_ref, outer_buf, local_sem.at[5]),
    ]
    for copy in local[:2]:
        copy.start()
    pl.semaphore_wait(barrier, len(peers) + 1 - outer)

    pieces = (pl.ds(0, half), pl.ds(half, half))
    direct = {}
    for turn in range(2):
        for d in (1, 2):
            piece = (d - 1 + turn) % 2
            direct[d, piece] = remote(
                cot_ref.at[pieces[piece]], cot_buf.at[d, pieces[piece]],
                send_sem.at[0], cot_recv.at[d - 1, piece], (rep, shards[d]),
            )
            direct[d, piece].start()

    for copy in local[2:] + finals:
        copy.start()

    def issue(i):
        at = units[i][2]
        for d in (3, 1, 2):
            remote(
                acts_ref.at[:, span(shards[d] * rows + at, size)], acts_buf.at[d, :, span(at, size)],
                send_sem.at[1], acts_recv.at[i], (rep, shards[d]),
            ).start()

    for i in range(EARLY):
        issue(i)
    relays = []
    for d, via in ((1, 2), (2, 1)):
        piece = d - 1
        direct[d, piece].wait_recv()
        relay = remote(
            cot_buf.at[d, pieces[piece]], cot_buf.at[3, pieces[piece]],
            send_sem.at[0], cot_recv.at[2, piece], (rep, shards[via]),
        )
        relay.start()
        relays.append(relay)
    for i in range(EARLY, AFTER):
        issue(i)
    for copy in local:
        copy.wait()
    for d in (1, 2):
        direct[d, 2 - d].wait_recv()
    for copy in relays:
        copy.wait_recv()
    for i in range(AFTER, WINDOW):
        issue(i)

    def arrival(slot, part):
        piece = far_in.at[slot, part]
        return remote(piece, piece, send_sem.at[3], far_recv.at[slot, part], (partner, shard))

    def forward(step):
        at_outer, at_inner = OUTER_PLAN[step], INNER_PLAN[step]
        slot, part = pick(at_outer[3], at_inner[3]), pick(at_outer[1], at_inner[1])
        line_to = pick(lines[at_outer[2]], lines[at_inner[2]])
        remote(
            far_out.at[step], far_in.at[slot, part], send_sem.at[3], far_recv.at[slot, part],
            (line_to * 2 + core, shard),
        ).start()

    def combine(step):
        slot, part = INNER_PLAN[step][4]

        @pl.when(is_inner)
        def _():
            arrival(slot, part).wait_recv()
            far_out[step] = (stash[step] + far_in[slot, part].astype(jnp.float32)).astype(jnp.bfloat16)
            forward(step)

    held = []
    for i, (step, h, at) in enumerate(units):
        rows_at = span(at, size)
        arrived = acts_buf.at[1:, :, rows_at]
        remote(arrived, arrived, send_sem.at[1], acts_recv.at[i], (rep, shards[1])).wait_recv()
        if h == 0 and i + WINDOW < len(units):
            issue(i + WINDOW)
        gradient = lax.dot_general(
            acts_buf[:, :, rows_at].reshape(tokens, size), cot_buf[...].reshape(tokens, width),
            (((0,), (0,)), ((), ())), preferred_element_type=jnp.float32,
        )
        value = adamw_direction(first_buf[rows_at, :], second_buf[rows_at, :], gradient)
        pairing = remote(
            pair_out.at[step], pair_in.at[step], send_sem.at[2], pair_recv.at[step], (partner, shard)
        )
        if h == 0:
            pair_out[step] = value
            pairing.start()
            while held:
                combine(held.pop())
            continue
        pairing.wait_recv()
        value = value + pair_in[step]
        part = OUTER_PLAN[step][1]
        if OUTER_PLAN[step][2] is None:
            stash[step] = value
        elif INNER_PLAN[step][4] is None:
            far_out[step] = value.astype(jnp.bfloat16)
            forward(step)
        else:
            held.append(step)

            @pl.when(is_inner)
            def _(value=value, step=step):
                stash[step] = value

            @pl.when(is_outer)
            def _(value=value, step=step):
                far_out[step] = value.astype(jnp.bfloat16)
                forward(step)

        if i + WINDOW < len(units):
            issue(i + WINDOW)
        if OUTER_PLAN[step][2] is not None:
            continue
        if part == 0:
            for copy in finals:
                copy.wait()

            @pl.when(is_inner)
            def _(value=value, step=step):
                arrival(2, 0).wait_recv()
                stash[step] = value + far_in[2, 0].astype(jnp.float32)

        arrival(0, part).wait_recv()
        arrival(1, part).wait_recv()
        here = pl.ds(part * size, size)
        total = stash[step] + (far_in[0, part].astype(jnp.float32) + far_in[1, part].astype(jnp.float32))
        anchor = anchor_buf[here, :]
        drift_mean = inner_rate * (total / n_rep + decay_rate * anchor)
        new_mom = momentum * outer_buf[here, :] + drift_mean
        new_params_ref[here, :] = anchor - outer_rate * (drift_mean + momentum * new_mom)
        new_mom_ref[here, :] = new_mom

    for j, sent in enumerate((cot_buf.at[1:], acts_buf.at[1:], pair_out, far_out)):
        remote(sent, sent, send_sem.at[j], send_sem.at[j], (partner, shard)).wait_send()

def fused_round(acts, cot, params, first, second, outer, n_rep, n_fsdp):
    tokens, width = cot.shape
    rows = first.shape[0]
    block = rows // n_rep
    size = block // 2
    steps = len(OUTER_PLAN)
    return pl.pallas_call(
        functools.partial(kernel, n_rep),
        out_shape=(pltpu.VMEM((block, width), jnp.float32),) * 2,
        in_specs=[pl.BlockSpec(memory_space=pltpu.HBM)] * 6,
        out_specs=(pl.BlockSpec(memory_space=pltpu.VMEM),) * 2,
        scratch_shapes=[
            pltpu.VMEM((n_fsdp, tokens, rows), jnp.bfloat16),
            pltpu.VMEM((n_fsdp, tokens, width), jnp.bfloat16),
            pltpu.VMEM((rows, width), jnp.float32),
            pltpu.VMEM((rows, width), jnp.float32),
            pltpu.VMEM((steps, size, width), jnp.float32),
            pltpu.VMEM((steps, size, width), jnp.float32),
            pltpu.VMEM((steps - 2, size, width), jnp.bfloat16),
            pltpu.VMEM((4, 2, size, width), jnp.bfloat16),
            pltpu.VMEM((steps, size, width), jnp.float32),
            pltpu.VMEM((block, width), jnp.float32),
            pltpu.VMEM((block, width), jnp.float32),
            pltpu.SemaphoreType.DMA((2 * steps,)),
            pltpu.SemaphoreType.DMA((3, 2)),
            pltpu.SemaphoreType.DMA((steps,)),
            pltpu.SemaphoreType.DMA((4, 2)),
            pltpu.SemaphoreType.DMA((4,)),
            pltpu.SemaphoreType.DMA((6,)),
        ],
        compiler_params=pltpu.CompilerParams(collective_id=0, has_side_effects=True),
    )(acts, cot, params, first, second, outer)

def plain_sum(acts, cot, first, second):
    inputs = lax.all_to_all(acts, "fsdp", split_axis=1, concat_axis=0, tiled=True)
    cots = lax.all_gather(cot, "fsdp", axis=0, tiled=True)
    gradient = lax.dot_general(
        inputs, cots, (((0,), (0,)), ((), ())), preferred_element_type=jnp.float32
    )
    return lax.psum_scatter(
        adamw_direction(first, second, gradient), "replica", scatter_dimension=0, tiled=True
    )

def per_device(n_rep, n_fsdp, acts, key_cot, params, moment_one, moment_two, outer_mom):
    block = params.shape[0] // n_rep
    acts, key_cot = acts[0], key_cot[0]
    if block % (2 * UNIT) == 0 and n_rep == 8 and n_fsdp == 4:
        return fused_round(acts, key_cot, params, moment_one, moment_two, outer_mom, n_rep, n_fsdp)
    total = plain_sum(acts, key_cot, moment_one, moment_two)
    anchor = lax.dynamic_slice_in_dim(params, lax.axis_index("replica") * block, block, 0)
    drift_mean = inner_rate * (total / n_rep + decay_rate * anchor)
    new_mom = momentum * outer_mom + drift_mean
    new_params = anchor - outer_rate * (drift_mean + momentum * new_mom)
    return (new_params, new_mom)

def solution(mesh):
    return jax.shard_map(
        functools.partial(per_device, mesh.shape["replica"], mesh.shape["fsdp"]),
        mesh=mesh,
        in_specs=(
            P(None, ("replica", "fsdp"), None),
            P(None, ("replica", "fsdp"), None),
            P("fsdp", None),
            P("fsdp", None),
            P("fsdp", None),
            P(("fsdp", "replica"), None),
        ),
        out_specs=(P(("fsdp", "replica"), None), P(("fsdp", "replica"), None)),
        check_vma=False,
    )
```

```python
import functools

import jax
import jax.numpy as jnp
from jax import lax
from jax.experimental import pallas as pl
from jax.experimental.pallas import tpu as pltpu
from jax.sharding import PartitionSpec as P

beta_one = 0.9
beta_two = 0.95
epsilon = 1e-08
inner_rate = 0.3
decay_rate = 0.1
outer_rate = 0.7
momentum = 0.9

MESH = pl.DeviceIdType.MESH
OUTER_PLAN = (
    (3, 0, 1, 3, None), (2, 0, 2, 2, None), (3, 1, 1, 3, None), (2, 1, 1, 2, None),
    (1, 0, 1, 0, None), (1, 1, 1, 0, None), (0, 0, None, None, None), (0, 1, None, None, None),
)
INNER_PLAN = (
    (3, 0, 3, 1, None), (1, 0, 1, 0, None), (2, 0, 2, 1, (3, 0)), (1, 1, 1, 0, None),
    (2, 1, 2, 1, (3, 1)), (3, 1, 3, 1, (2, 1)), (0, 0, None, None, None), (0, 1, None, None, None),
)
UNIT = 128
WINDOW = 5
EARLY = 1
PIECES = 2
AFTER = 4

def adamw_direction(first, second, gradient):
    first = beta_one * first + (1.0 - beta_one) * gradient
    second = beta_two * second + (1.0 - beta_two) * gradient * gradient
    return first / (jnp.sqrt(second) + epsilon)

def kernel(
    n_rep,
    acts_ref, cot_ref, params_ref, first_ref, second_ref, outer_ref, new_params_ref, new_mom_ref,
    acts_buf, cot_buf, first_buf, second_buf, pair_out, pair_in, far_out, far_in, stash, anchor_buf, outer_buf,
    acts_recv, cot_recv, pair_recv, far_recv, send_sem, local_sem,
):
    rep = lax.axis_index("replica")
    shard = lax.axis_index("fsdp")
    line, core = lax.div(rep, 2), lax.rem(rep, 2)
    row_at, col_at = lax.div(shard, 2), lax.rem(shard, 2)
    rows = first_ref.shape[0]
    block = rows // n_rep
    size = block // 2
    half = cot_ref.shape[0] // 2
    tokens = acts_buf.shape[0] * acts_buf.shape[1]
    width = cot_buf.shape[2]
    partner = line * 2 + (1 - core)
    shards = (shard, row_at * 2 + (1 - col_at), (1 - row_at) * 2 + col_at, (1 - row_at) * 2 + (1 - col_at))
    lines = (line, line + 1 - 2 * lax.rem(line, 2), lax.rem(line + 2, 4), 3 - line)
    outer = 1 - lax.rem(lax.div(line, 2) + lax.rem(line, 2), 2)
    is_outer = outer == 1
    is_inner = jnp.logical_not(is_outer)

    def span(start, length):
        return pl.ds(pl.multiple_of(start, length), length)

    def remote(source, target, send, recv, device):
        return pltpu.make_async_remote_copy(
            src_ref=source, dst_ref=target, send_sem=send, recv_sem=recv, device_id=device, device_id_type=MESH
        )

    def pick(at_outer, at_inner):
        return outer * at_outer + (1 - outer) * at_inner

    units = []
    for step, (at_outer, at_inner) in enumerate(zip(OUTER_PLAN, INNER_PLAN)):
        other = pick(lines[at_outer[0]], lines[at_inner[0]])
        start = pick(at_outer[1], at_inner[1]) * size
        for h, owner in ((0, 1 - core), (1, core)):
            units.append((step, h, (other * 2 + owner) * block + start))

    barrier = pltpu.get_barrier_semaphore()
    peers = [(rep, shards[d]) for d in (3, 1, 2)] + [(partner, shard)]
    peers += [(lines[o] * 2 + core, shard) for o in (1, 2)]
    for peer in peers:
        pl.semaphore_signal(barrier, inc=1, device_id=peer, device_id_type=MESH)

    @pl.when(is_inner)
    def _():
        pl.semaphore_signal(barrier, inc=1, device_id=(lines[3] * 2 + core, shard), device_id_type=MESH)

    local = [
        pltpu.make_async_copy(cot_ref, cot_buf.at[0], local_sem.at[0]),
        pltpu.make_async_copy(acts_ref.at[:, span(shard * rows, rows)], acts_buf.at[0], local_sem.at[1]),
        pltpu.make_async_copy(first_ref, first_buf, local_sem.at[2]),
        pltpu.make_async_copy(second_ref, second_buf, local_sem.at[3]),
    ]
    finals = [
        pltpu.make_async_copy(params_ref.at[span(rep * block, block)], anchor_buf, local_sem.at[4]),
        pltpu.make_async_copy(outer_ref, outer_buf, local_sem.at[5]),
    ]
    for copy in local[:2]:
        copy.start()
    pl.semaphore_wait(barrier, len(peers) + 1 - outer)

    pieces = (pl.ds(0, half), pl.ds(half, half))
    direct = {}
    for turn in range(2):
        for d in (1, 2):
            piece = (d - 1 + turn) % 2
            direct[d, piece] = remote(
                cot_ref.at[pieces[piece]], cot_buf.at[d, pieces[piece]],
                send_sem.at[0], cot_recv.at[d - 1, piece], (rep, shards[d]),
            )
            direct[d, piece].start()

    for copy in local[2:] + finals:
        copy.start()

    def issue(i):
        at = units[i][2]
        for d in (3, 1, 2):
            remote(
                acts_ref.at[:, span(shards[d] * rows + at, size)], acts_buf.at[d, :, span(at, size)],
                send_sem.at[1], acts_recv.at[i], (rep, shards[d]),
            ).start()

    for i in range(EARLY):
        issue(i)
    relays = []
    for d, via in ((1, 2), (2, 1)):
        piece = d - 1
        direct[d, piece].wait_recv()
        relay = remote(
            cot_buf.at[d, pieces[piece]], cot_buf.at[3, pieces[piece]],
            send_sem.at[0], cot_recv.at[2, piece], (rep, shards[via]),
        )
        relay.start()
        relays.append(relay)
    for i in range(EARLY, AFTER):
        issue(i)
    for copy in local:
        copy.wait()
    for d in (1, 2):
        direct[d, 2 - d].wait_recv()
    for copy in relays:
        copy.wait_recv()
    for i in range(AFTER, WINDOW):
        issue(i)

    def arrival(slot, part):
        piece = far_in.at[slot, part]
        return remote(piece, piece, send_sem.at[3], far_recv.at[slot, part], (partner, shard))

    def forward(step):
        at_outer, at_inner = OUTER_PLAN[step], INNER_PLAN[step]
        slot, part = pick(at_outer[3], at_inner[3]), pick(at_outer[1], at_inner[1])
        line_to = pick(lines[at_outer[2]], lines[at_inner[2]])
        remote(
            far_out.at[step], far_in.at[slot, part], send_sem.at[3], far_recv.at[slot, part],
            (line_to * 2 + core, shard),
        ).start()

    def combine(step):
        slot, part = INNER_PLAN[step][4]

        @pl.when(is_inner)
        def _():
            arrival(slot, part).wait_recv()
            far_out[step] = (stash[step] + far_in[slot, part].astype(jnp.float32)).astype(jnp.bfloat16)
            forward(step)

    held = []
    for i, (step, h, at) in enumerate(units):
        rows_at = span(at, size)
        arrived = acts_buf.at[1:, :, rows_at]
        remote(arrived, arrived, send_sem.at[1], acts_recv.at[i], (rep, shards[1])).wait_recv()
        if h == 0 and i + WINDOW < len(units):
            issue(i + WINDOW)
        gradient = lax.dot_general(
            acts_buf[:, :, rows_at].reshape(tokens, size), cot_buf[...].reshape(tokens, width),
            (((0,), (0,)), ((), ())), preferred_element_type=jnp.float32,
        )
        value = adamw_direction(first_buf[rows_at, :], second_buf[rows_at, :], gradient)
        pairing = remote(
            pair_out.at[step], pair_in.at[step], send_sem.at[2], pair_recv.at[step], (partner, shard)
        )
        if h == 0:
            pair_out[step] = value
            pairing.start()
            while held:
                combine(held.pop())
            continue
        pairing.wait_recv()
        value = value + pair_in[step]
        part = OUTER_PLAN[step][1]
        if OUTER_PLAN[step][2] is None:
            stash[step] = value
        elif INNER_PLAN[step][4] is None:
            far_out[step] = value.astype(jnp.bfloat16)
            forward(step)
        else:
            held.append(step)

            @pl.when(is_inner)
            def _(value=value, step=step):
                stash[step] = value

            @pl.when(is_outer)
            def _(value=value, step=step):
                far_out[step] = value.astype(jnp.bfloat16)
                forward(step)

        if i + WINDOW < len(units):
            issue(i + WINDOW)
        if OUTER_PLAN[step][2] is not None:
            continue
        if part == 0:
            for copy in finals:
                copy.wait()

            @pl.when(is_inner)
            def _(value=value, step=step):
                arrival(2, 0).wait_recv()
                stash[step] = value + far_in[2, 0].astype(jnp.float32)

        arrival(0, part).wait_recv()
        arrival(1, part).wait_recv()
        here = pl.ds(part * size, size)
        total = stash[step] + (far_in[0, part].astype(jnp.float32) + far_in[1, part].astype(jnp.float32))
        anchor = anchor_buf[here, :]
        drift_mean = inner_rate * (total / n_rep + decay_rate * anchor)
        new_mom = momentum * outer_buf[here, :] + drift_mean
        new_params_ref[here, :] = anchor - outer_rate * (drift_mean + momentum * new_mom)
        new_mom_ref[here, :] = new_mom

    for j, sent in enumerate((cot_buf.at[1:], acts_buf.at[1:], pair_out, far_out)):
        remote(sent, sent, send_sem.at[j], send_sem.at[j], (partner, shard)).wait_send()

def write_out(params_ref, mom_ref, out_params_ref, out_mom_ref, sem):
    rows = params_ref.shape[0] // PIECES
    copies = []
    for j, (source, target) in enumerate(((params_ref, out_params_ref), (mom_ref, out_mom_ref))):
        for p in range(PIECES):
            piece = pl.ds(p * rows, rows)
            copies.append(pltpu.make_async_copy(source.at[piece], target.at[piece], sem.at[j, p]))
            copies[-1].start()
    for copy in copies:
        copy.wait()

def fused_round(acts, cot, params, first, second, outer, n_rep, n_fsdp):
    tokens, width = cot.shape
    rows = first.shape[0]
    block = rows // n_rep
    size = block // 2
    steps = len(OUTER_PLAN)
    results = pl.pallas_call(
        functools.partial(kernel, n_rep),
        out_shape=(pltpu.VMEM((block, width), jnp.float32),) * 2,
        in_specs=[pl.BlockSpec(memory_space=pltpu.HBM)] * 6,
        out_specs=(pl.BlockSpec(memory_space=pltpu.VMEM),) * 2,
        scratch_shapes=[
            pltpu.VMEM((n_fsdp, tokens, rows), jnp.bfloat16),
            pltpu.VMEM((n_fsdp, tokens, width), jnp.bfloat16),
            pltpu.VMEM((rows, width), jnp.float32),
            pltpu.VMEM((rows, width), jnp.float32),
            pltpu.VMEM((steps, size, width), jnp.float32),
            pltpu.VMEM((steps, size, width), jnp.float32),
            pltpu.VMEM((steps - 2, size, width), jnp.bfloat16),
            pltpu.VMEM((4, 2, size, width), jnp.bfloat16),
            pltpu.VMEM((steps, size, width), jnp.float32),
            pltpu.VMEM((block, width), jnp.float32),
            pltpu.VMEM((block, width), jnp.float32),
            pltpu.SemaphoreType.DMA((2 * steps,)),
            pltpu.SemaphoreType.DMA((3, 2)),
            pltpu.SemaphoreType.DMA((steps,)),
            pltpu.SemaphoreType.DMA((4, 2)),
            pltpu.SemaphoreType.DMA((4,)),
            pltpu.SemaphoreType.DMA((6,)),
        ],
        compiler_params=pltpu.CompilerParams(collective_id=0, has_side_effects=True),
    )(acts, cot, params, first, second, outer)
    return pl.pallas_call(
        write_out,
        out_shape=(jax.ShapeDtypeStruct((block, width), jnp.float32),) * 2,
        in_specs=[pl.BlockSpec(memory_space=pltpu.VMEM)] * 2,
        out_specs=(pl.BlockSpec(memory_space=pltpu.HBM),) * 2,
        scratch_shapes=[pltpu.SemaphoreType.DMA((2, PIECES))],
        compiler_params=pltpu.CompilerParams(vmem_limit_bytes=16 * block * width),
    )(*results)

def plain_sum(acts, cot, first, second):
    inputs = lax.all_to_all(acts, "fsdp", split_axis=1, concat_axis=0, tiled=True)
    cots = lax.all_gather(cot, "fsdp", axis=0, tiled=True)
    gradient = lax.dot_general(
        inputs, cots, (((0,), (0,)), ((), ())), preferred_element_type=jnp.float32
    )
    return lax.psum_scatter(
        adamw_direction(first, second, gradient), "replica", scatter_dimension=0, tiled=True
    )

def per_device(n_rep, n_fsdp, acts, key_cot, params, moment_one, moment_two, outer_mom):
    block = params.shape[0] // n_rep
    acts, key_cot = acts[0], key_cot[0]
    if block % (2 * UNIT) == 0 and n_rep == 8 and n_fsdp == 4:
        return fused_round(acts, key_cot, params, moment_one, moment_two, outer_mom, n_rep, n_fsdp)
    total = plain_sum(acts, key_cot, moment_one, moment_two)
    anchor = lax.dynamic_slice_in_dim(params, lax.axis_index("replica") * block, block, 0)
    drift_mean = inner_rate * (total / n_rep + decay_rate * anchor)
    new_mom = momentum * outer_mom + drift_mean
    new_params = anchor - outer_rate * (drift_mean + momentum * new_mom)
    return (new_params, new_mom)

def solution(mesh):
    return jax.shard_map(
        functools.partial(per_device, mesh.shape["replica"], mesh.shape["fsdp"]),
        mesh=mesh,
        in_specs=(
            P(None, ("replica", "fsdp"), None),
            P(None, ("replica", "fsdp"), None),
            P("fsdp", None),
            P("fsdp", None),
            P("fsdp", None),
            P(("fsdp", "replica"), None),
        ),
        out_specs=(P(("fsdp", "replica"), None), P(("fsdp", "replica"), None)),
        check_vma=False,
    )
```

```python
import functools

import jax
import jax.numpy as jnp
from jax import lax
from jax.experimental import pallas as pl
from jax.experimental.pallas import tpu as pltpu
from jax.sharding import PartitionSpec as P

beta_one = 0.9
beta_two = 0.95
epsilon = 1e-08
inner_rate = 0.3
decay_rate = 0.1
outer_rate = 0.7
momentum = 0.9

MESH = pl.DeviceIdType.MESH
OUTER_PLAN = (
    (3, 0, 1, 3, None), (2, 0, 2, 2, None), (3, 1, 1, 3, None), (2, 1, 1, 2, None),
    (1, 0, 1, 0, None), (1, 1, 1, 0, None), (0, 0, None, None, None), (0, 1, None, None, None),
)
INNER_PLAN = (
    (3, 0, 3, 1, None), (1, 0, 1, 0, None), (2, 0, 2, 1, (3, 0)), (1, 1, 1, 0, None),
    (2, 1, 2, 1, (3, 1)), (3, 1, 3, 1, (2, 1)), (0, 0, None, None, None), (0, 1, None, None, None),
)
UNIT = 128
WINDOW = 6
EARLY = 1
PIECES = 1
AFTER = 4

def adamw_direction(first, second, gradient):
    first = beta_one * first + (1.0 - beta_one) * gradient
    second = beta_two * second + (1.0 - beta_two) * gradient * gradient
    return first / (jnp.sqrt(second) + epsilon)

def kernel(
    n_rep,
    acts_ref, cot_ref, params_ref, first_ref, second_ref, outer_ref, new_params_ref, new_mom_ref,
    acts_buf, cot_buf, first_buf, second_buf, pair_out, pair_in, far_out, far_in, stash, anchor_buf, outer_buf,
    acts_recv, cot_recv, pair_recv, far_recv, send_sem, local_sem,
):
    rep = lax.axis_index("replica")
    shard = lax.axis_index("fsdp")
    line, core = lax.div(rep, 2), lax.rem(rep, 2)
    row_at, col_at = lax.div(shard, 2), lax.rem(shard, 2)
    rows = first_ref.shape[0]
    block = rows // n_rep
    size = block // 2
    half = cot_ref.shape[0] // 2
    tokens = acts_buf.shape[0] * acts_buf.shape[1]
    width = cot_buf.shape[2]
    partner = line * 2 + (1 - core)
    shards = (shard, row_at * 2 + (1 - col_at), (1 - row_at) * 2 + col_at, (1 - row_at) * 2 + (1 - col_at))
    lines = (line, line + 1 - 2 * lax.rem(line, 2), lax.rem(line + 2, 4), 3 - line)
    outer = 1 - lax.rem(lax.div(line, 2) + lax.rem(line, 2), 2)
    is_outer = outer == 1
    is_inner = jnp.logical_not(is_outer)

    def span(start, length):
        return pl.ds(pl.multiple_of(start, length), length)

    def remote(source, target, send, recv, device):
        return pltpu.make_async_remote_copy(
            src_ref=source, dst_ref=target, send_sem=send, recv_sem=recv, device_id=device, device_id_type=MESH
        )

    def pick(at_outer, at_inner):
        return outer * at_outer + (1 - outer) * at_inner

    units = []
    for step, (at_outer, at_inner) in enumerate(zip(OUTER_PLAN, INNER_PLAN)):
        other = pick(lines[at_outer[0]], lines[at_inner[0]])
        start = pick(at_outer[1], at_inner[1]) * size
        for h, owner in ((0, 1 - core), (1, core)):
            units.append((step, h, (other * 2 + owner) * block + start))

    barrier = pltpu.get_barrier_semaphore()
    peers = [(rep, shards[d]) for d in (3, 1, 2)] + [(partner, shard)]
    peers += [(lines[o] * 2 + core, shard) for o in (1, 2)]
    for peer in peers:
        pl.semaphore_signal(barrier, inc=1, device_id=peer, device_id_type=MESH)

    @pl.when(is_inner)
    def _():
        pl.semaphore_signal(barrier, inc=1, device_id=(lines[3] * 2 + core, shard), device_id_type=MESH)

    local = [
        pltpu.make_async_copy(cot_ref, cot_buf.at[0], local_sem.at[0]),
        pltpu.make_async_copy(acts_ref.at[:, span(shard * rows, rows)], acts_buf.at[0], local_sem.at[1]),
        pltpu.make_async_copy(first_ref, first_buf, local_sem.at[2]),
        pltpu.make_async_copy(second_ref, second_buf, local_sem.at[3]),
    ]
    finals = [
        pltpu.make_async_copy(params_ref.at[span(rep * block, block)], anchor_buf, local_sem.at[4]),
        pltpu.make_async_copy(outer_ref, outer_buf, local_sem.at[5]),
    ]
    for copy in local + finals:
        copy.start()
    pl.semaphore_wait(barrier, len(peers) + 1 - outer)

    local[0].wait()
    pieces = (pl.ds(0, half), pl.ds(half, half))
    direct = {}
    for turn in range(2):
        for d in (1, 2):
            piece = (d - 1 + turn) % 2
            direct[d, piece] = remote(
                cot_buf.at[0, pieces[piece]], cot_buf.at[d, pieces[piece]],
                send_sem.at[0], cot_recv.at[d - 1, piece], (rep, shards[d]),
            )
            direct[d, piece].start()

    def issue(i):
        at = units[i][2]
        for d in (3, 1, 2):
            remote(
                acts_ref.at[:, span(shards[d] * rows + at, size)], acts_buf.at[d, :, span(at, size)],
                send_sem.at[1], acts_recv.at[i], (rep, shards[d]),
            ).start()

    for i in range(EARLY):
        issue(i)
    relays = []
    for d, via in ((1, 2), (2, 1)):
        piece = d - 1
        direct[d, piece].wait_recv()
        relay = remote(
            cot_buf.at[d, pieces[piece]], cot_buf.at[3, pieces[piece]],
            send_sem.at[0], cot_recv.at[2, piece], (rep, shards[via]),
        )
        relay.start()
        relays.append(relay)
    for i in range(EARLY, AFTER):
        issue(i)
    for copy in local[1:]:
        copy.wait()
    for d in (1, 2):
        direct[d, 2 - d].wait_recv()
    for copy in relays:
        copy.wait_recv()
    for i in range(AFTER, WINDOW):
        issue(i)

    def arrival(slot, part):
        piece = far_in.at[slot, part]
        return remote(piece, piece, send_sem.at[3], far_recv.at[slot, part], (partner, shard))

    def forward(step):
        at_outer, at_inner = OUTER_PLAN[step], INNER_PLAN[step]
        slot, part = pick(at_outer[3], at_inner[3]), pick(at_outer[1], at_inner[1])
        line_to = pick(lines[at_outer[2]], lines[at_inner[2]])
        remote(
            far_out.at[step], far_in.at[slot, part], send_sem.at[3], far_recv.at[slot, part],
            (line_to * 2 + core, shard),
        ).start()

    def combine(step):
        slot, part = INNER_PLAN[step][4]

        @pl.when(is_inner)
        def _():
            arrival(slot, part).wait_recv()
            far_out[step] = (stash[step] + far_in[slot, part].astype(jnp.float32)).astype(jnp.bfloat16)
            forward(step)

    held = []
    for i, (step, h, at) in enumerate(units):
        rows_at = span(at, size)
        arrived = acts_buf.at[1:, :, rows_at]
        remote(arrived, arrived, send_sem.at[1], acts_recv.at[i], (rep, shards[1])).wait_recv()
        if h == 0 and i + WINDOW < len(units):
            issue(i + WINDOW)
        gradient = lax.dot_general(
            acts_buf[:, :, rows_at].reshape(tokens, size), cot_buf[...].reshape(tokens, width),
            (((0,), (0,)), ((), ())), preferred_element_type=jnp.float32,
        )
        value = adamw_direction(first_buf[rows_at, :], second_buf[rows_at, :], gradient)
        pairing = remote(
            pair_out.at[step], pair_in.at[step], send_sem.at[2], pair_recv.at[step], (partner, shard)
        )
        if h == 0:
            pair_out[step] = value
            pairing.start()
            while held:
                combine(held.pop())
            continue
        pairing.wait_recv()
        value = value + pair_in[step]
        part = OUTER_PLAN[step][1]
        if OUTER_PLAN[step][2] is None:
            stash[step] = value
        elif INNER_PLAN[step][4] is None:
            far_out[step] = value.astype(jnp.bfloat16)
            forward(step)
        else:
            held.append(step)

            @pl.when(is_inner)
            def _(value=value, step=step):
                stash[step] = value

            @pl.when(is_outer)
            def _(value=value, step=step):
                far_out[step] = value.astype(jnp.bfloat16)
                forward(step)

        if i + WINDOW < len(units):
            issue(i + WINDOW)
        if OUTER_PLAN[step][2] is not None:
            continue
        if part == 0:
            for copy in finals:
                copy.wait()

            @pl.when(is_inner)
            def _(value=value, step=step):
                arrival(2, 0).wait_recv()
                stash[step] = value + far_in[2, 0].astype(jnp.float32)

        arrival(0, part).wait_recv()
        arrival(1, part).wait_recv()
        here = pl.ds(part * size, size)
        total = stash[step] + (far_in[0, part].astype(jnp.float32) + far_in[1, part].astype(jnp.float32))
        anchor = anchor_buf[here, :]
        drift_mean = inner_rate * (total / n_rep + decay_rate * anchor)
        new_mom = momentum * outer_buf[here, :] + drift_mean
        new_params_ref[here, :] = anchor - outer_rate * (drift_mean + momentum * new_mom)
        new_mom_ref[here, :] = new_mom

    for j, sent in enumerate((cot_buf.at[1:], acts_buf.at[1:], pair_out, far_out)):
        remote(sent, sent, send_sem.at[j], send_sem.at[j], (partner, shard)).wait_send()

def write_out(params_ref, mom_ref, out_params_ref, out_mom_ref, sem):
    rows = params_ref.shape[0] // PIECES
    copies = []
    for j, (source, target) in enumerate(((params_ref, out_params_ref), (mom_ref, out_mom_ref))):
        for p in range(PIECES):
            piece = pl.ds(p * rows, rows)
            copies.append(pltpu.make_async_copy(source.at[piece], target.at[piece], sem.at[j, p]))
            copies[-1].start()
    for copy in copies:
        copy.wait()

def fused_round(acts, cot, params, first, second, outer, n_rep, n_fsdp):
    tokens, width = cot.shape
    rows = first.shape[0]
    block = rows // n_rep
    size = block // 2
    steps = len(OUTER_PLAN)
    results = pl.pallas_call(
        functools.partial(kernel, n_rep),
        out_shape=(pltpu.VMEM((block, width), jnp.float32),) * 2,
        in_specs=[pl.BlockSpec(memory_space=pltpu.HBM)] * 6,
        out_specs=(pl.BlockSpec(memory_space=pltpu.VMEM),) * 2,
        scratch_shapes=[
            pltpu.VMEM((n_fsdp, tokens, rows), jnp.bfloat16),
            pltpu.VMEM((n_fsdp, tokens, width), jnp.bfloat16),
            pltpu.VMEM((rows, width), jnp.float32),
            pltpu.VMEM((rows, width), jnp.float32),
            pltpu.VMEM((steps, size, width), jnp.float32),
            pltpu.VMEM((steps, size, width), jnp.float32),
            pltpu.VMEM((steps - 2, size, width), jnp.bfloat16),
            pltpu.VMEM((4, 2, size, width), jnp.bfloat16),
            pltpu.VMEM((steps, size, width), jnp.float32),
            pltpu.VMEM((block, width), jnp.float32),
            pltpu.VMEM((block, width), jnp.float32),
            pltpu.SemaphoreType.DMA((2 * steps,)),
            pltpu.SemaphoreType.DMA((3, 2)),
            pltpu.SemaphoreType.DMA((steps,)),
            pltpu.SemaphoreType.DMA((4, 2)),
            pltpu.SemaphoreType.DMA((4,)),
            pltpu.SemaphoreType.DMA((6,)),
        ],
        compiler_params=pltpu.CompilerParams(collective_id=0, has_side_effects=True),
    )(acts, cot, params, first, second, outer)
    return pl.pallas_call(
        write_out,
        out_shape=(jax.ShapeDtypeStruct((block, width), jnp.float32),) * 2,
        in_specs=[pl.BlockSpec(memory_space=pltpu.VMEM)] * 2,
        out_specs=(pl.BlockSpec(memory_space=pltpu.HBM),) * 2,
        scratch_shapes=[pltpu.SemaphoreType.DMA((2, PIECES))],
        compiler_params=pltpu.CompilerParams(vmem_limit_bytes=16 * block * width),
    )(*results)

def plain_sum(acts, cot, first, second):
    inputs = lax.all_to_all(acts, "fsdp", split_axis=1, concat_axis=0, tiled=True)
    cots = lax.all_gather(cot, "fsdp", axis=0, tiled=True)
    gradient = lax.dot_general(
        inputs, cots, (((0,), (0,)), ((), ())), preferred_element_type=jnp.float32
    )
    return lax.psum_scatter(
        adamw_direction(first, second, gradient), "replica", scatter_dimension=0, tiled=True
    )

def per_device(n_rep, n_fsdp, acts, key_cot, params, moment_one, moment_two, outer_mom):
    block = params.shape[0] // n_rep
    acts, key_cot = acts[0], key_cot[0]
    if block % (2 * UNIT) == 0 and n_rep == 8 and n_fsdp == 4:
        return fused_round(acts, key_cot, params, moment_one, moment_two, outer_mom, n_rep, n_fsdp)
    total = plain_sum(acts, key_cot, moment_one, moment_two)
    anchor = lax.dynamic_slice_in_dim(params, lax.axis_index("replica") * block, block, 0)
    drift_mean = inner_rate * (total / n_rep + decay_rate * anchor)
    new_mom = momentum * outer_mom + drift_mean
    new_params = anchor - outer_rate * (drift_mean + momentum * new_mom)
    return (new_params, new_mom)

def solution(mesh):
    return jax.shard_map(
        functools.partial(per_device, mesh.shape["replica"], mesh.shape["fsdp"]),
        mesh=mesh,
        in_specs=(
            P(None, ("replica", "fsdp"), None),
            P(None, ("replica", "fsdp"), None),
            P("fsdp", None),
            P("fsdp", None),
            P("fsdp", None),
            P(("fsdp", "replica"), None),
        ),
        out_specs=(P(("fsdp", "replica"), None), P(("fsdp", "replica"), None)),
        check_vma=False,
    )
```

```python
import functools

import jax
import jax.numpy as jnp
from jax import lax
from jax.experimental import pallas as pl
from jax.experimental.pallas import tpu as pltpu
from jax.sharding import PartitionSpec as P

beta_one = 0.9
beta_two = 0.95
epsilon = 1e-08
inner_rate = 0.3
decay_rate = 0.1
outer_rate = 0.7
momentum = 0.9

MESH = pl.DeviceIdType.MESH
OUTER_PLAN = (
    (3, 0, 1, 3, None), (2, 0, 2, 2, None), (3, 1, 1, 3, None), (2, 1, 1, 2, None),
    (1, 0, 1, 0, None), (1, 1, 1, 0, None), (0, 0, None, None, None), (0, 1, None, None, None),
)
INNER_PLAN = (
    (3, 0, 3, 1, None), (1, 0, 1, 0, None), (2, 0, 2, 1, (3, 0)), (1, 1, 1, 0, None),
    (2, 1, 2, 1, (3, 1)), (3, 1, 3, 1, (2, 1)), (0, 0, None, None, None), (0, 1, None, None, None),
)
UNIT = 128
WINDOW = 6
EARLY = 1
PIECES = 1
AFTER = 4

def adamw_direction(first, second, gradient):
    first = beta_one * first + (1.0 - beta_one) * gradient
    second = beta_two * second + (1.0 - beta_two) * gradient * gradient
    return first / (jnp.sqrt(second) + epsilon)

def kernel(
    n_rep,
    acts_ref, cot_ref, params_ref, first_ref, second_ref, outer_ref, new_params_ref, new_mom_ref,
    acts_buf, cot_buf, first_buf, second_buf, pair_out, pair_in, far_out, far_in, stash, anchor_buf, outer_buf,
    acts_recv, cot_recv, pair_recv, far_recv, send_sem, local_sem,
):
    rep = lax.axis_index("replica")
    shard = lax.axis_index("fsdp")
    line, core = lax.div(rep, 2), lax.rem(rep, 2)
    row_at, col_at = lax.div(shard, 2), lax.rem(shard, 2)
    rows = first_ref.shape[0]
    block = rows // n_rep
    size = block // 2
    half = cot_ref.shape[0] // 2
    tokens = acts_buf.shape[0] * acts_buf.shape[1]
    width = cot_buf.shape[2]
    partner = line * 2 + (1 - core)
    shards = (shard, row_at * 2 + (1 - col_at), (1 - row_at) * 2 + col_at, (1 - row_at) * 2 + (1 - col_at))
    lines = (line, line + 1 - 2 * lax.rem(line, 2), lax.rem(line + 2, 4), 3 - line)
    outer = 1 - lax.rem(lax.div(line, 2) + lax.rem(line, 2), 2)
    is_outer = outer == 1
    is_inner = jnp.logical_not(is_outer)

    def span(start, length):
        return pl.ds(pl.multiple_of(start, length), length)

    def remote(source, target, send, recv, device):
        return pltpu.make_async_remote_copy(
            src_ref=source, dst_ref=target, send_sem=send, recv_sem=recv, device_id=device, device_id_type=MESH
        )

    def pick(at_outer, at_inner):
        return outer * at_outer + (1 - outer) * at_inner

    units = []
    for step, (at_outer, at_inner) in enumerate(zip(OUTER_PLAN, INNER_PLAN)):
        other = pick(lines[at_outer[0]], lines[at_inner[0]])
        start = pick(at_outer[1], at_inner[1]) * size
        for h, owner in ((0, 1 - core), (1, core)):
            units.append((step, h, (other * 2 + owner) * block + start))

    barrier = pltpu.get_barrier_semaphore()
    peers = [(rep, shards[d]) for d in (3, 1, 2)] + [(partner, shard)]
    peers += [(lines[o] * 2 + core, shard) for o in (1, 2)]
    for peer in peers:
        pl.semaphore_signal(barrier, inc=1, device_id=peer, device_id_type=MESH)

    @pl.when(is_inner)
    def _():
        pl.semaphore_signal(barrier, inc=1, device_id=(lines[3] * 2 + core, shard), device_id_type=MESH)

    local = [
        pltpu.make_async_copy(cot_ref, cot_buf.at[0], local_sem.at[0]),
        pltpu.make_async_copy(acts_ref.at[:, span(shard * rows, rows)], acts_buf.at[0], local_sem.at[1]),
        pltpu.make_async_copy(first_ref, first_buf, local_sem.at[2]),
        pltpu.make_async_copy(second_ref, second_buf, local_sem.at[3]),
    ]
    finals = [
        pltpu.make_async_copy(params_ref.at[span(rep * block, block)], anchor_buf, local_sem.at[4]),
        pltpu.make_async_copy(outer_ref, outer_buf, local_sem.at[5]),
    ]
    for copy in local + finals:
        copy.start()
    pl.semaphore_wait(barrier, len(peers) + 1 - outer)

    local[0].wait()
    pieces = (pl.ds(0, half), pl.ds(half, half))
    direct = {}
    for turn in range(2):
        for d in (1, 2):
            piece = (d - 1 + turn) % 2
            direct[d, piece] = remote(
                cot_buf.at[0, pieces[piece]], cot_buf.at[d, pieces[piece]],
                send_sem.at[0], cot_recv.at[d - 1, piece], (rep, shards[d]),
            )
            direct[d, piece].start()

    def issue(i):
        at = units[i][2]
        for d in (3, 1, 2):
            remote(
                acts_ref.at[:, span(shards[d] * rows + at, size)], acts_buf.at[d, :, span(at, size)],
                send_sem.at[1], acts_recv.at[i], (rep, shards[d]),
            ).start()

    for i in range(EARLY):
        issue(i)
    relays = []
    for d, via in ((1, 2), (2, 1)):
        piece = d - 1
        direct[d, piece].wait_recv()
        relay = remote(
            cot_buf.at[d, pieces[piece]], cot_buf.at[3, pieces[piece]],
            send_sem.at[0], cot_recv.at[2, piece], (rep, shards[via]),
        )
        relay.start()
        relays.append(relay)
    for i in range(EARLY, AFTER):
        issue(i)
    for copy in local[1:]:
        copy.wait()
    for d in (1, 2):
        direct[d, 2 - d].wait_recv()
    for copy in relays:
        copy.wait_recv()
    for i in range(AFTER, WINDOW):
        issue(i)

    def arrival(slot, part):
        piece = far_in.at[slot, part]
        return remote(piece, piece, send_sem.at[3], far_recv.at[slot, part], (partner, shard))

    def forward(step):
        at_outer, at_inner = OUTER_PLAN[step], INNER_PLAN[step]
        slot, part = pick(at_outer[3], at_inner[3]), pick(at_outer[1], at_inner[1])
        line_to = pick(lines[at_outer[2]], lines[at_inner[2]])
        remote(
            far_out.at[step], far_in.at[slot, part], send_sem.at[3], far_recv.at[slot, part],
            (line_to * 2 + core, shard),
        ).start()

    def combine(step):
        slot, part = INNER_PLAN[step][4]

        @pl.when(is_inner)
        def _():
            arrival(slot, part).wait_recv()
            far_out[step] = (stash[step] + far_in[slot, part].astype(jnp.float32)).astype(jnp.bfloat16)
            forward(step)

    held = []
    for i, (step, h, at) in enumerate(units):
        rows_at = span(at, size)
        arrived = acts_buf.at[1:, :, rows_at]
        remote(arrived, arrived, send_sem.at[1], acts_recv.at[i], (rep, shards[1])).wait_recv()
        gradient = lax.dot_general(
            acts_buf[:, :, rows_at].reshape(tokens, size), cot_buf[...].reshape(tokens, width),
            (((0,), (0,)), ((), ())), preferred_element_type=jnp.float32,
        )
        value = adamw_direction(first_buf[rows_at, :], second_buf[rows_at, :], gradient)
        pairing = remote(
            pair_out.at[step], pair_in.at[step], send_sem.at[2], pair_recv.at[step], (partner, shard)
        )
        if h == 0:
            pair_out[step] = value
            pairing.start()
            while held:
                combine(held.pop())
            if i + WINDOW < len(units):
                issue(i + WINDOW)
            continue
        pairing.wait_recv()
        value = value + pair_in[step]
        part = OUTER_PLAN[step][1]
        if OUTER_PLAN[step][2] is None:
            stash[step] = value
        elif INNER_PLAN[step][4] is None:
            far_out[step] = value.astype(jnp.bfloat16)
            forward(step)
        else:
            held.append(step)

            @pl.when(is_inner)
            def _(value=value, step=step):
                stash[step] = value

            @pl.when(is_outer)
            def _(value=value, step=step):
                far_out[step] = value.astype(jnp.bfloat16)
                forward(step)

        if i + WINDOW < len(units):
            issue(i + WINDOW)
        if OUTER_PLAN[step][2] is not None:
            continue
        if part == 0:
            for copy in finals:
                copy.wait()

            @pl.when(is_inner)
            def _(value=value, step=step):
                arrival(2, 0).wait_recv()
                stash[step] = value + far_in[2, 0].astype(jnp.float32)

        arrival(0, part).wait_recv()
        arrival(1, part).wait_recv()
        here = pl.ds(part * size, size)
        total = stash[step] + (far_in[0, part].astype(jnp.float32) + far_in[1, part].astype(jnp.float32))
        anchor = anchor_buf[here, :]
        drift_mean = inner_rate * (total / n_rep + decay_rate * anchor)
        new_mom = momentum * outer_buf[here, :] + drift_mean
        new_params_ref[here, :] = anchor - outer_rate * (drift_mean + momentum * new_mom)
        new_mom_ref[here, :] = new_mom

    for j, sent in enumerate((cot_buf.at[1:], acts_buf.at[1:], pair_out, far_out)):
        remote(sent, sent, send_sem.at[j], send_sem.at[j], (partner, shard)).wait_send()

def write_out(params_ref, mom_ref, out_params_ref, out_mom_ref, sem):
    rows = params_ref.shape[0] // PIECES
    copies = []
    for j, (source, target) in enumerate(((params_ref, out_params_ref), (mom_ref, out_mom_ref))):
        for p in range(PIECES):
            piece = pl.ds(p * rows, rows)
            copies.append(pltpu.make_async_copy(source.at[piece], target.at[piece], sem.at[j, p]))
            copies[-1].start()
    for copy in copies:
        copy.wait()

def fused_round(acts, cot, params, first, second, outer, n_rep, n_fsdp):
    tokens, width = cot.shape
    rows = first.shape[0]
    block = rows // n_rep
    size = block // 2
    steps = len(OUTER_PLAN)
    results = pl.pallas_call(
        functools.partial(kernel, n_rep),
        out_shape=(pltpu.VMEM((block, width), jnp.float32),) * 2,
        in_specs=[pl.BlockSpec(memory_space=pltpu.HBM)] * 6,
        out_specs=(pl.BlockSpec(memory_space=pltpu.VMEM),) * 2,
        scratch_shapes=[
            pltpu.VMEM((n_fsdp, tokens, rows), jnp.bfloat16),
            pltpu.VMEM((n_fsdp, tokens, width), jnp.bfloat16),
            pltpu.VMEM((rows, width), jnp.float32),
            pltpu.VMEM((rows, width), jnp.float32),
            pltpu.VMEM((steps, size, width), jnp.float32),
            pltpu.VMEM((steps, size, width), jnp.float32),
            pltpu.VMEM((steps - 2, size, width), jnp.bfloat16),
            pltpu.VMEM((4, 2, size, width), jnp.bfloat16),
            pltpu.VMEM((steps, size, width), jnp.float32),
            pltpu.VMEM((block, width), jnp.float32),
            pltpu.VMEM((block, width), jnp.float32),
            pltpu.SemaphoreType.DMA((2 * steps,)),
            pltpu.SemaphoreType.DMA((3, 2)),
            pltpu.SemaphoreType.DMA((steps,)),
            pltpu.SemaphoreType.DMA((4, 2)),
            pltpu.SemaphoreType.DMA((4,)),
            pltpu.SemaphoreType.DMA((6,)),
        ],
        compiler_params=pltpu.CompilerParams(collective_id=0, has_side_effects=True),
    )(acts, cot, params, first, second, outer)
    return pl.pallas_call(
        write_out,
        out_shape=(jax.ShapeDtypeStruct((block, width), jnp.float32),) * 2,
        in_specs=[pl.BlockSpec(memory_space=pltpu.VMEM)] * 2,
        out_specs=(pl.BlockSpec(memory_space=pltpu.HBM),) * 2,
        scratch_shapes=[pltpu.SemaphoreType.DMA((2, PIECES))],
        compiler_params=pltpu.CompilerParams(vmem_limit_bytes=16 * block * width),
    )(*results)

def plain_sum(acts, cot, first, second):
    inputs = lax.all_to_all(acts, "fsdp", split_axis=1, concat_axis=0, tiled=True)
    cots = lax.all_gather(cot, "fsdp", axis=0, tiled=True)
    gradient = lax.dot_general(
        inputs, cots, (((0,), (0,)), ((), ())), preferred_element_type=jnp.float32
    )
    return lax.psum_scatter(
        adamw_direction(first, second, gradient), "replica", scatter_dimension=0, tiled=True
    )

def per_device(n_rep, n_fsdp, acts, key_cot, params, moment_one, moment_two, outer_mom):
    block = params.shape[0] // n_rep
    acts, key_cot = acts[0], key_cot[0]
    if block % (2 * UNIT) == 0 and n_rep == 8 and n_fsdp == 4:
        return fused_round(acts, key_cot, params, moment_one, moment_two, outer_mom, n_rep, n_fsdp)
    total = plain_sum(acts, key_cot, moment_one, moment_two)
    anchor = lax.dynamic_slice_in_dim(params, lax.axis_index("replica") * block, block, 0)
    drift_mean = inner_rate * (total / n_rep + decay_rate * anchor)
    new_mom = momentum * outer_mom + drift_mean
    new_params = anchor - outer_rate * (drift_mean + momentum * new_mom)
    return (new_params, new_mom)

def solution(mesh):
    return jax.shard_map(
        functools.partial(per_device, mesh.shape["replica"], mesh.shape["fsdp"]),
        mesh=mesh,
        in_specs=(
            P(None, ("replica", "fsdp"), None),
            P(None, ("replica", "fsdp"), None),
            P("fsdp", None),
            P("fsdp", None),
            P("fsdp", None),
            P(("fsdp", "replica"), None),
        ),
        out_specs=(P(("fsdp", "replica"), None), P(("fsdp", "replica"), None)),
        check_vma=False,
    )
```
